32 devices in a mesh: section: 2 (over x), dp: 16 (over z, y, core).
Axes of the slice: x: 2, y: 2, z: 4, core: 2. Of those that a mesh axis runs over, the one named last changes fastest.
Arguments:
- inputs: bfloat16 [4, 2048, 1536], P(None, 'dp'), may hold values from -6 to 6
- out_grad: bfloat16 [4, 2048, 1536], P(None, 'dp'), may hold values from -0.125 to 0.125
- guide_bin: int32 [4, 1], replicated, may hold values from 0 to 31
- time_step: int32 [4, 1], replicated, may hold values from 0 to 999
- guide_table: bfloat16 [32, 4608], replicated, may hold values from -3 to 3
- section_table: float32 [2, 3, 1536], P('section'), may hold values from -3 to 3
- value_weight: bfloat16 [2, 1536, 1536], P('section'), may hold values from -0.15625 to 0.15625
- proj_weight: bfloat16 [2, 1536, 1536], P('section'), may hold values from -0.15625 to 0.15625
Outputs:
- value_grad: float32 [2, 1536, 1536], P('section', 'dp')
- proj_grad: float32 [2, 1536, 1536], P('section', 'dp')
- table_grad: float32 [2, 3, 1536], P('section', None, 'dp')
The draws below stay inside these ranges and needn't reach their ends.
All inputs are finite; a program needn't handle non-finite values.
Results may differ from the reference program's by a relative error of at most 0.017.
Values may be sent and summed in bfloat16 or wider, within the bound.
A program may use at most 128 MiB of HBM per device.

```python
import math
import jax
import jax.numpy as jnp
from jax import lax

D = 1536
H = 1536
MICRO = 4
BINS = 32
STEPS = 1000
TOKENS = 2048
SAMPLES = 1
BLOCKS = 2


def plant(drawn, own_key, least, high):
    dims = drawn.shape
    spot = [jax.random.randint(jax.random.fold_in(own_key, axis), (), 0, dims[axis]) for axis in range(len(dims))]
    drawn = drawn.at[tuple(spot)].set(least)
    longest = dims.index(max(dims))
    spot[longest] = (spot[longest] + 1) % dims[longest]
    return drawn.at[tuple(spot)].set(high)


def levels(key, extent, cuts, least, top_value):
    def one(axis_at, blocks):
        steps = jax.random.uniform(jax.random.fold_in(jax.random.fold_in(key, 6), axis_at), (blocks,), jnp.float32, least / len(cuts), top_value / len(cuts))
        return jnp.repeat(jnp.exp(steps), extent[axis_at] // blocks).reshape((-1,) + (1,) * (len(extent) - axis_at - 1))

    factor_of = one(*cuts[0])
    for cut in cuts[1:]:
        factor_of = factor_of * one(*cut)
    return factor_of


def normal_values(stream_key, extent, deviation, bound, pieces=(), kind=jnp.bfloat16):
    array = jax.random.normal(stream_key, extent, jnp.float32) * deviation
    if len(pieces) > 0:
        array = levels(stream_key, extent, pieces, -0.22, 0.18) * array
    return jnp.clip(array, min=-bound, max=bound).astype(kind)


def setup_inputs(seed: int = 0) -> dict:
    arg_keys = jax.random.split(jax.random.key(seed), 9)
    inputs = normal_values(arg_keys[0], (MICRO, TOKENS, D), 1.0, 6.0, ((1, 16),))
    out_grad = normal_values(arg_keys[1], (MICRO, TOKENS, D), TOKENS ** -0.5, 0.125, ((1, 16),))
    guide_bin = plant(jax.random.randint(arg_keys[2], (MICRO, SAMPLES), 0, BINS), jax.random.fold_in(arg_keys[2], 1), 0, BINS - 1).astype(jnp.int32)
    time_step = plant(jax.random.randint(arg_keys[3], (MICRO, SAMPLES), 0, STEPS), jax.random.fold_in(arg_keys[3], 1), 0, STEPS - 1).astype(jnp.int32)
    guide_table = normal_values(arg_keys[4], (BINS, 3 * D), 0.5, 3.0)
    section_table = normal_values(arg_keys[5], (BLOCKS, 3, D), 0.5, 3.0, ((0, 2),), jnp.float32)
    value_weight = normal_values(arg_keys[6], (BLOCKS, D, H), D ** -0.5, 0.15625, ((0, 2),))
    proj_weight = normal_values(arg_keys[7], (BLOCKS, H, D), H ** -0.5, 0.15625, ((0, 2),))
    return {"inputs": inputs, "out_grad": out_grad, "guide_bin": guide_bin, "time_step": time_step, "guide_table": guide_table, "section_table": section_table, "value_weight": value_weight, "proj_weight": proj_weight}


NORM_FLOOR = 0.1

def normalize(hidden):
    centre = lax.optimization_barrier(jnp.mean(hidden, axis=-1, keepdims=True))
    centred = hidden - centre
    spread = lax.optimization_barrier(jnp.mean(centred * centred, axis=-1, keepdims=True))
    inverse = lax.rsqrt(spread + NORM_FLOOR)
    return (centred * inverse, inverse)

def conditions(guide_bin, time_step, guide_table):
    total = guide_table.shape[1]
    half = total // 2
    frequency = jnp.exp(-math.log(10000.0) * jnp.arange(half, dtype=jnp.float32) / half)
    angle = time_step.astype(jnp.float32)[..., None] * frequency
    waves = jnp.concatenate([jnp.sin(angle), jnp.cos(angle)], axis=-1)
    return guide_table.astype(jnp.float32)[guide_bin] + 0.5 * waves

def forward_block(block_in, modulation, value_weight, proj_weight):
    width = block_in.shape[1]
    hidden = block_in.astype(jnp.float32)
    normed, inverse = normalize(hidden)
    shift = modulation[:, :width]
    scale = modulation[:, width:2 * width]
    gate = modulation[:, 2 * width:]
    modulated = (normed * (1.0 + scale) + shift).astype(jnp.bfloat16)
    values = jnp.dot(modulated, value_weight, preferred_element_type=jnp.float32).astype(jnp.bfloat16)
    projected = jnp.dot(values, proj_weight, preferred_element_type=jnp.float32)
    block_out = (hidden + gate * projected).astype(jnp.bfloat16)
    return (block_out, modulated, values, projected)

def backward_block(block_in, modulated, values, projected, upstream, modulation, value_weight, proj_weight):
    width = block_in.shape[1]
    hidden = block_in.astype(jnp.float32)
    normed, inverse = normalize(hidden)
    scale = modulation[:, width:2 * width]
    gate = modulation[:, 2 * width:]
    grad_up = upstream.astype(jnp.float32)
    grad_proj = (gate * grad_up).astype(jnp.bfloat16)
    part_proj = jnp.dot(values.T, grad_proj, preferred_element_type=jnp.float32)
    grad_values = jnp.dot(grad_proj, proj_weight.T, preferred_element_type=jnp.float32).astype(jnp.bfloat16)
    part_value = jnp.dot(modulated.T, grad_values, preferred_element_type=jnp.float32)
    grad_mod = jnp.dot(grad_values, value_weight.T, preferred_element_type=jnp.float32)
    part_table = jnp.stack([lax.optimization_barrier(jnp.sum(grad_mod, axis=0)), lax.optimization_barrier(jnp.sum(grad_mod * normed, axis=0)), lax.optimization_barrier(jnp.sum(grad_up * projected, axis=0))])
    grad_norm = grad_mod * (1.0 + scale)
    centre_grad = lax.optimization_barrier(jnp.mean(grad_norm, axis=-1, keepdims=True))
    cross = lax.optimization_barrier(jnp.mean(grad_norm * normed, axis=-1, keepdims=True))
    grad_in = grad_up + inverse * (grad_norm - centre_grad - normed * cross)
    return (grad_in.astype(jnp.bfloat16), part_value, part_proj, part_table)

def reference(inputs, out_grad, guide_bin, time_step, guide_table, section_table, value_weight, proj_weight):
    condition = conditions(guide_bin, time_step, guide_table)
    rows_per = TOKENS // SAMPLES
    saved = []
    shared_all = []
    for batch in range(MICRO):
        shared = jnp.repeat(condition[batch], rows_per, axis=0)
        shared_all.append(shared)
        block_in = inputs[batch]
        kept = []
        for block in range(BLOCKS):
            modulation = shared + section_table[block].reshape(-1)
            kept.append(block_in)
            block_in = forward_block(block_in, modulation, value_weight[block], proj_weight[block])[0]
        saved.append(kept)
    value_sums = [jnp.zeros((D, H), jnp.float32) for index in range(BLOCKS)]
    proj_sums = [jnp.zeros((H, D), jnp.float32) for index in range(BLOCKS)]
    table_sums = [jnp.zeros((3, D), jnp.float32) for index in range(BLOCKS)]
    for batch in range(MICRO):
        upstream = out_grad[batch]
        for block in range(BLOCKS - 1, -1, -1):
            modulation = shared_all[batch] + section_table[block].reshape(-1)
            block_in = saved[batch][block]
            block_out, modulated, values, projected = forward_block(block_in, modulation, value_weight[block], proj_weight[block])
            upstream, part_value, part_proj, part_table = backward_block(block_in, modulated, values, projected, upstream, modulation, value_weight[block], proj_weight[block])
            value_sums[block] = value_sums[block] + part_value
            proj_sums[block] = proj_sums[block] + part_proj
            table_sums[block] = table_sums[block] + part_table
    return (jnp.stack(value_sums), jnp.stack(proj_sums), jnp.stack(table_sums))
```

```python
import functools
import math

import jax
import jax.numpy as jnp
from jax import lax
from jax.experimental import pallas as pl
from jax.experimental.pallas import tpu as pltpu
from jax.sharding import PartitionSpec as P

NORM_FLOOR = 0.1


def shifted(value, axis, steps):
    count = lax.axis_size(axis)
    leading, last = (max(0, -steps), min(count, count - steps))
    return lax.ppermute(value, axis, [(source, source + steps) for source in range(leading, last)])


def normalize(hidden):
    centre = jnp.mean(hidden, axis=-1, keepdims=True)
    centred = hidden - centre
    spread = jnp.mean(centred * centred, axis=-1, keepdims=True)
    inverse = lax.rsqrt(spread + NORM_FLOOR)
    return (centred * inverse, inverse)


def conditions(guide_bin, time_step, guide_table):
    total = guide_table.shape[1]
    half = total // 2
    frequency = jnp.exp(-math.log(10000.0) * jnp.arange(half, dtype=jnp.float32) / half)
    angle = time_step.astype(jnp.float32)[..., None] * frequency
    waves = jnp.concatenate([jnp.sin(angle), jnp.cos(angle)], axis=-1)
    bin_count = guide_table.shape[0]
    onehot = (guide_bin[..., None] == jnp.arange(bin_count, dtype=jnp.int32)).astype(jnp.float32)
    picked = jnp.einsum(
        "msb,bw->msw", onehot, guide_table.astype(jnp.float32), precision=lax.Precision.HIGHEST
    )
    return picked + 0.5 * waves


def contract_rows(left, right):
    return lax.dot_general(
        left, right, (((0,), (0,)), ((), ())), preferred_element_type=jnp.float32
    )


def forward_block(block_in, modulation, value_weight, proj_weight):
    width = block_in.shape[1]
    hidden = block_in.astype(jnp.float32)
    normed, inverse = normalize(hidden)
    shift = modulation[:, :width]
    scale = modulation[:, width : 2 * width]
    gate = modulation[:, 2 * width :]
    modulated = (normed * (1.0 + scale) + shift).astype(jnp.bfloat16)
    values = jnp.dot(modulated, value_weight, preferred_element_type=jnp.float32).astype(
        jnp.bfloat16
    )
    projected = jnp.dot(values, proj_weight, preferred_element_type=jnp.float32)
    block_out = (hidden + gate * projected).astype(jnp.bfloat16)
    return (block_out, modulated, values, projected)


def backward_block(block_in, projected, upstream, modulation, value_weight, proj_weight):
    width = block_in.shape[1]
    hidden = block_in.astype(jnp.float32)
    normed, inverse = normalize(hidden)
    scale = modulation[:, width : 2 * width]
    gate = modulation[:, 2 * width :]
    grad_up = upstream.astype(jnp.float32)
    grad_proj = (gate * grad_up).astype(jnp.bfloat16)
    grad_values = lax.dot_general(
        grad_proj, proj_weight, (((1,), (1,)), ((), ())), preferred_element_type=jnp.float32
    ).astype(jnp.bfloat16)
    grad_mod = lax.dot_general(
        grad_values, value_weight, (((1,), (1,)), ((), ())), preferred_element_type=jnp.float32
    )
    part_table = jnp.stack(
        [
            jnp.sum(grad_mod, axis=0),
            jnp.sum(grad_mod * normed, axis=0),
            jnp.sum(grad_up * projected, axis=0),
        ]
    )
    grad_norm = grad_mod * (1.0 + scale)
    centre_grad = jnp.mean(grad_norm, axis=-1, keepdims=True)
    cross = jnp.mean(grad_norm * normed, axis=-1, keepdims=True)
    grad_in = grad_up + inverse * (grad_norm - centre_grad - normed * cross)
    return (grad_in.astype(jnp.bfloat16), grad_values, grad_proj, part_table)


def per_device_scan(
    inputs, out_grad, guide_bin, time_step, guide_table, section_table, value_weight, proj_weight
):
    sections = lax.axis_size("section")
    section_id = lax.axis_index("section")
    position = lax.axis_index("dp")
    group_size = lax.axis_size("dp")
    tok_dev = inputs.shape[1]
    width = inputs.shape[2]
    value_width = value_weight.shape[2]
    batches = inputs.shape[0]
    samples = guide_bin.shape[1]
    tokens = tok_dev * group_size
    rows_per = tokens // samples
    parts = 1
    unit_rows = tok_dev // parts
    units = batches * parts
    condition = conditions(guide_bin, time_step, guide_table)
    weights_value = value_weight[0]
    weights_proj = proj_weight[0]
    section_row = section_table[0].reshape(-1)
    sample_ids = jnp.arange(samples, dtype=jnp.int32)

    def unit_modulation(unit_id):
        batch_id = unit_id // parts
        piece_id = unit_id % parts
        chosen = lax.dynamic_index_in_dim(condition, batch_id, 0, keepdims=False)
        global_rows = (
            position * tok_dev + piece_id * unit_rows + jnp.arange(unit_rows, dtype=jnp.int32)
        )
        owner = global_rows // rows_per
        onehot = (owner[:, None] == sample_ids[None, :]).astype(jnp.float32)
        picked = jnp.dot(
            onehot, chosen, precision=lax.Precision.HIGHEST, preferred_element_type=jnp.float32
        )
        return picked + section_row

    slots = units + 1
    keep_in = jnp.zeros((slots, unit_rows, width), jnp.bfloat16)
    keep_mod = jnp.zeros((slots, unit_rows, width), jnp.bfloat16)
    keep_val = jnp.zeros((slots, unit_rows, value_width), jnp.bfloat16)
    keep_proj = jnp.zeros((slots, unit_rows, width), jnp.float32)
    arriving = jnp.zeros((unit_rows, width), jnp.bfloat16)

    def forward_tick(carry, tick_id):
        incoming, saved_in, saved_mod, saved_val, saved_proj = carry
        unit_id = tick_id - section_id
        valid = (unit_id >= 0) & (unit_id < units)
        clipped = jnp.clip(unit_id, 0, units - 1)
        first = lax.dynamic_index_in_dim(inputs, clipped, 0, keepdims=False)
        block_in = jnp.where(section_id == 0, first, incoming)

        def forward_active(operand):
            return forward_block(operand, unit_modulation(clipped), weights_value, weights_proj)

        def forward_resting(operand):
            return (
                jnp.zeros_like(operand),
                jnp.zeros_like(operand),
                jnp.zeros((unit_rows, value_width), jnp.bfloat16),
                jnp.zeros((unit_rows, width), jnp.float32),
            )

        block_out, modulated, values, projected = lax.cond(
            valid, forward_active, forward_resting, block_in
        )
        slot_id = jnp.where(valid, unit_id, units)
        saved_in = lax.dynamic_update_index_in_dim(saved_in, block_in, slot_id, 0)
        saved_mod = lax.dynamic_update_index_in_dim(saved_mod, modulated, slot_id, 0)
        saved_val = lax.dynamic_update_index_in_dim(saved_val, values, slot_id, 0)
        saved_proj = lax.dynamic_update_index_in_dim(saved_proj, projected, slot_id, 0)
        sent = shifted(block_out, "section", 1)
        return ((sent, saved_in, saved_mod, saved_val, saved_proj), None)

    ticks = jnp.arange(units + sections - 1, dtype=jnp.int32)
    carry, unused = lax.scan(
        forward_tick, (arriving, keep_in, keep_mod, keep_val, keep_proj), ticks
    )
    arriving, keep_in, keep_mod, keep_val, keep_proj = carry
    store = jnp.zeros((slots, unit_rows, value_width), jnp.bfloat16)
    extra_zero = jnp.zeros((unit_rows, value_width), jnp.bfloat16)
    keep_grad = jnp.zeros((slots, unit_rows, width), jnp.bfloat16)
    proj_sum = jnp.zeros((value_width, width), jnp.float32)
    table_sum = jnp.zeros((3, width), jnp.float32)

    def backward_tick(carry, tick_id):
        incoming, store_now, grads_now, proj_now, table_now = carry
        unit_id = tick_id - (sections - 1 - section_id)
        valid = (unit_id >= 0) & (unit_id < units)
        clipped = jnp.clip(unit_id, 0, units - 1)
        last = lax.dynamic_index_in_dim(out_grad, clipped, 0, keepdims=False)
        upstream = jnp.where(section_id == sections - 1, last, incoming)
        block_in = lax.dynamic_index_in_dim(keep_in, clipped, 0, keepdims=False)
        modulated = lax.dynamic_index_in_dim(keep_mod, clipped, 0, keepdims=False)
        values = lax.dynamic_index_in_dim(keep_val, clipped, 0, keepdims=False)
        projected = lax.dynamic_index_in_dim(keep_proj, clipped, 0, keepdims=False)

        def backward_active(operand):
            grad_in, grad_values, grad_proj, part_table = backward_block(
                block_in, projected, operand, unit_modulation(clipped), weights_value, weights_proj
            )
            part_proj = jnp.zeros((value_width, width), jnp.float32)
            return (grad_in, grad_values, grad_proj, part_proj, part_table)

        def backward_resting(operand):
            return (
                jnp.zeros_like(operand),
                extra_zero,
                jnp.zeros((unit_rows, width), jnp.bfloat16),
                jnp.zeros((value_width, width), jnp.float32),
                jnp.zeros((3, width), jnp.float32),
            )

        grad_in, extra, grad_proj, part_proj, part_table = lax.cond(
            valid, backward_active, backward_resting, upstream
        )
        slot_id = jnp.where(valid, unit_id, units)
        store_now = lax.dynamic_update_index_in_dim(store_now, extra, slot_id, 0)
        grads_now = lax.dynamic_update_index_in_dim(grads_now, grad_proj, slot_id, 0)
        sent = shifted(grad_in, "section", -1)
        return ((sent, store_now, grads_now, proj_now + part_proj, table_now + part_table), None)

    carry, unused = lax.scan(
        backward_tick, (arriving, store, keep_grad, proj_sum, table_sum), ticks
    )
    arriving, store, keep_grad, proj_sum, table_sum = carry
    mod_rows = keep_mod[:units].reshape(units * unit_rows, width)
    grad_rows = store[:units].reshape(units * unit_rows, value_width)
    columns = mod_rows
    value_part = lax.psum_scatter(
        contract_rows(columns, grad_rows), "dp", scatter_dimension=0, tiled=True
    )
    val_rows = keep_val[:units].reshape(units * unit_rows, value_width)
    upper_rows = keep_grad[:units].reshape(units * unit_rows, width)
    columns = val_rows
    proj_part = lax.psum_scatter(
        contract_rows(columns, upper_rows), "dp", scatter_dimension=0, tiled=True
    )
    table_part = lax.psum_scatter(table_sum, "dp", scatter_dimension=1, tiled=True)
    return (value_part[None], proj_part[None], table_part[None])


MESH = pl.DeviceIdType.MESH


def scatter_kernel(far, value_ref, proj_ref, table_ref, value_out, proj_out, table_out,
                   core_in, own, side_out, side_in, far_out, far_in, table_in,
                   core_send, core_recv, side_send, side_recv, far_send, far_recv,
                   table_send, table_recv):
    group = 4 * far
    me = lax.axis_index("dp")
    core, side, place = me % 2, (me // 2) % 2, me // 4
    barrier = pltpu.get_barrier_semaphore()
    for step in range(1, group):
        pl.semaphore_signal(
            barrier, inc=1, device_id={"dp": (me + step) % group}, device_id_type=MESH
        )
    pl.semaphore_wait(barrier, group - 1)

    matrices = (proj_ref, value_ref)
    offsets = [(far // 2 + step) % far for step in range(far)]
    offsets = [offset for offset in offsets if offset] + [0]
    pieces = [(matrix, slot) for matrix in range(2) for slot in range(far)]

    def row(slot, which_side, which_core):
        return (((place + offsets[slot]) % far) * 2 + which_side) * 2 + which_core

    core_copies = {}
    for turn in range(2):
        for index, (matrix, slot) in enumerate(pieces):
            which = (1 - side) if turn == 0 else side
            copy = pltpu.make_async_remote_copy(
                src_ref=matrices[matrix].at[row(slot, which, 1 - core)],
                dst_ref=core_in.at[turn, index],
                send_sem=core_send.at[turn, index],
                recv_sem=core_recv.at[turn, index],
                device_id={"dp": me - core + (1 - core)},
                device_id_type=MESH,
            )
            copy.start()
            core_copies[turn, index] = copy
    table_copies = []
    for step in range(1, group):
        copy = pltpu.make_async_remote_copy(
            src_ref=table_ref.at[(me + step) % group],
            dst_ref=table_in.at[step - 1],
            send_sem=table_send.at[step - 1],
            recv_sem=table_recv.at[step - 1],
            device_id={"dp": (me + step) % group},
            device_id_type=MESH,
        )
        copy.start()
        table_copies.append(copy)

    side_copies = []
    for index, (matrix, slot) in enumerate(pieces):
        core_copies[0, index].wait_recv()
        mine = matrices[matrix][row(slot, 1 - side, core)].astype(jnp.float32)
        side_out[index] = (mine + core_in[0, index].astype(jnp.float32)).astype(jnp.bfloat16)
        copy = pltpu.make_async_remote_copy(
            src_ref=side_out.at[index],
            dst_ref=side_in.at[index],
            send_sem=side_send.at[index],
            recv_sem=side_recv.at[index],
            device_id={"dp": me + 2 - 4 * side},
            device_id_type=MESH,
        )
        copy.start()
        side_copies.append(copy)
    far_copies = {}
    for index, (matrix, slot) in enumerate(pieces):
        core_copies[1, index].wait_recv()
        mine = matrices[matrix][row(slot, side, core)].astype(jnp.float32)
        mine = mine + core_in[1, index].astype(jnp.float32)
        side_copies[index].wait_recv()
        mine = mine + side_in[index].astype(jnp.float32)
        if offsets[slot] == 0:
            own[matrix] = mine
        else:
            far_out[index] = mine.astype(jnp.bfloat16)
            copy = pltpu.make_async_remote_copy(
                src_ref=far_out.at[index],
                dst_ref=far_in.at[index],
                send_sem=far_send.at[index],
                recv_sem=far_recv.at[index],
                device_id={"dp": (me + 4 * offsets[slot]) % group},
                device_id_type=MESH,
            )
            copy.start()
            far_copies[index] = copy
    total = table_ref[me]
    for step in range(1, group):
        table_copies[step - 1].wait_recv()
        total = total + table_in[step - 1]
    table_out[...] = total
    for matrix, out in enumerate((proj_out, value_out)):
        result = own[matrix]
        for index, (which, slot) in enumerate(pieces):
            if which == matrix and index in far_copies:
                far_copies[index].wait_recv()
                result = result + far_in[index].astype(jnp.float32)
        out[...] = result
    for copy in list(core_copies.values()) + table_copies + side_copies:
        copy.wait_send()
    for copy in far_copies.values():
        copy.wait_send()


def scatter_sums(value_part, proj_part, table_part):
    group = lax.axis_size("dp")
    far = group // 4
    rows, width = value_part.shape[0] // group, value_part.shape[1]
    table_rows, lanes = table_part.shape[0], table_part.shape[1] // group
    tables = table_part.reshape(table_rows, group, lanes).transpose(1, 0, 2)
    tables = jnp.pad(tables, ((0, 0), (0, -table_rows % 8), (0, -lanes % 128)))
    count = 2 * far
    block = (rows, width)
    vmem = pl.BlockSpec(memory_space=pltpu.VMEM)
    dma = pltpu.SemaphoreType.DMA
    value_sum, proj_sum, table_sum = pl.pallas_call(
        functools.partial(scatter_kernel, far),
        out_shape=(
            jax.ShapeDtypeStruct(block, jnp.float32),
            jax.ShapeDtypeStruct((value_part.shape[0] // group, proj_part.shape[1]), jnp.float32),
            jax.ShapeDtypeStruct(tables.shape[1:], jnp.float32),
        ),
        in_specs=[vmem] * 3,
        out_specs=(vmem,) * 3,
        scratch_shapes=[
            pltpu.VMEM((2, count) + block, jnp.bfloat16),
            pltpu.VMEM((2,) + block, jnp.float32),
            pltpu.VMEM((count,) + block, jnp.bfloat16),
            pltpu.VMEM((count,) + block, jnp.bfloat16),
            pltpu.VMEM((count,) + block, jnp.bfloat16),
            pltpu.VMEM((count,) + block, jnp.bfloat16),
            pltpu.VMEM((group - 1,) + tables.shape[1:], jnp.float32),
            dma((2, count)), dma((2, count)), dma((count,)), dma((count,)),
            dma((count,)), dma((count,)), dma((group - 1,)), dma((group - 1,)),
        ],
        compiler_params=pltpu.CompilerParams(
            collective_id=0, has_side_effects=True, vmem_limit_bytes=56 * 1024 * 1024
        ),
    )(
        value_part.reshape((group,) + block),
        proj_part.reshape((group,) + block),
        tables,
    )
    return value_sum, proj_sum, table_sum[:table_rows, :lanes]


def modulation_rows(guide_bin, time_step, guide_table, section_row, tok_dev):
    group_size = lax.axis_size("dp")
    position = lax.axis_index("dp")
    batches, samples = guide_bin.shape
    rows_per = tok_dev * group_size // samples
    if rows_per % tok_dev == 0:
        owner = (position * tok_dev) // rows_per
        guide_bin = lax.dynamic_slice_in_dim(guide_bin, owner, 1, 1)
        time_step = lax.dynamic_slice_in_dim(time_step, owner, 1, 1)
    kept = guide_bin.shape[1]
    total = guide_table.shape[1]
    half = total // 2
    frequency = jnp.exp(-math.log(10000.0) * jnp.arange(half, dtype=jnp.float32) / half)
    angle = time_step.reshape(-1, 1).astype(jnp.float32) * frequency
    waves = jnp.concatenate([jnp.sin(angle), jnp.cos(angle)], axis=-1)
    bins = jnp.arange(guide_table.shape[0], dtype=jnp.int32)
    picked = jnp.sum(
        jnp.where(
            (guide_bin.reshape(-1, 1) == bins)[:, :, None], guide_table.astype(jnp.float32), 0.0
        ),
        axis=1,
    )
    rows = (picked + 0.5 * waves + section_row).reshape(batches, kept, total)
    if kept == samples and samples > 1:
        owners = (position * tok_dev + jnp.arange(tok_dev, dtype=jnp.int32)) // rows_per
        rows = jnp.take(rows, owners, axis=1)
    return rows


def dot_rows(left, right, contract):
    units, rows, depth = left.shape
    out = lax.dot_general(
        left.reshape(units * rows, depth), right, (((1,), (contract,)), ((), ())),
        preferred_element_type=jnp.float32,
    )
    return out.reshape(units, rows, out.shape[1])


def forward_units(block_in, modulation, value_weight, proj_weight):
    width = block_in.shape[2]
    hidden = block_in.astype(jnp.float32)
    normed, inverse = normalize(hidden)
    shift, scale, gate = (modulation[:, :, i * width : (i + 1) * width] for i in range(3))
    modulated = (normed * (1.0 + scale) + shift).astype(jnp.bfloat16)
    values = dot_rows(modulated, value_weight, 0).astype(jnp.bfloat16)
    projected = dot_rows(values, proj_weight, 0)
    block_out = (hidden + gate * projected).astype(jnp.bfloat16)
    return block_out, modulated, values, projected


def backward_units(block_in, projected, upstream, modulation, value_weight, proj_weight):
    width = block_in.shape[2]
    hidden = block_in.astype(jnp.float32)
    normed, inverse = normalize(hidden)
    scale, gate = (modulation[:, :, i * width : (i + 1) * width] for i in (1, 2))
    grad_up = upstream.astype(jnp.float32)
    grad_proj = (gate * grad_up).astype(jnp.bfloat16)
    grad_values = dot_rows(grad_proj, proj_weight, 1).astype(jnp.bfloat16)
    grad_mod = dot_rows(grad_values, value_weight, 1)
    part_table = jnp.stack(
        [
            jnp.sum(grad_mod, axis=(0, 1)),
            jnp.sum(grad_mod * normed, axis=(0, 1)),
            jnp.sum(grad_up * projected, axis=(0, 1)),
        ]
    )
    grad_norm = grad_mod * (1.0 + scale)
    centre_grad = jnp.mean(grad_norm, axis=-1, keepdims=True)
    cross = jnp.mean(grad_norm * normed, axis=-1, keepdims=True)
    grad_in = grad_up + inverse * (grad_norm - centre_grad - normed * cross)
    return grad_in.astype(jnp.bfloat16), grad_values, grad_proj, part_table


def per_device(
    inputs, out_grad, guide_bin, time_step, guide_table, section_table, value_weight, proj_weight
):
    if lax.axis_size("section") != 2 or lax.axis_size("dp") % 4:
        return per_device_scan(
            inputs, out_grad, guide_bin, time_step, guide_table, section_table,
            value_weight, proj_weight,
        )
    first = lax.axis_index("section") == 0
    batches, tok_dev, width = inputs.shape
    weights = (value_weight[0], proj_weight[0])
    modulation = modulation_rows(
        guide_bin, time_step, guide_table, section_table[0].reshape(-1), tok_dev
    )
    out0, modulated0, values0, projected0 = forward_units(inputs, modulation, *weights)
    later = []
    returned = []
    for unit in range(batches):
        part = slice(unit, unit + 1)
        arrived = shifted(out0[part], "section", 1)
        unit_mod = modulation[part]
        unused, modulated, values, projected = forward_units(arrived, unit_mod, *weights)
        grad_in, grad_values, grad_proj, table = backward_units(
            arrived, projected, out_grad[part], unit_mod, *weights
        )
        returned.append(shifted(grad_in, "section", -1))
        later.append((modulated, values, grad_values, grad_proj, table))
    earlier = []
    for part in (slice(0, batches - 1), slice(batches - 1, batches)):
        if part.stop > part.start:
            unused, grad_values, grad_proj, table = backward_units(
                inputs[part], projected0[part], jnp.concatenate(returned[part], axis=0),
                modulation[part], *weights
            )
            earlier.append((grad_values, grad_proj, table))

    def rows_of(mine, theirs):
        chosen = jnp.where(first, mine, jnp.concatenate(theirs, axis=0))
        return chosen.reshape(batches * tok_dev, chosen.shape[2])

    modulated, values, grad_values, grad_proj, tables = zip(*later)
    grad_values0, grad_proj0, tables0 = zip(*earlier)
    mod_rows = rows_of(modulated0, modulated)
    val_rows = rows_of(values0, values)
    grad_rows = rows_of(jnp.concatenate(grad_values0, axis=0), grad_values)
    upper_rows = rows_of(jnp.concatenate(grad_proj0, axis=0), grad_proj)
    table_part = jnp.where(first, sum(tables0), sum(tables))
    value_part = contract_rows(mod_rows, grad_rows).astype(jnp.bfloat16)
    proj_part = contract_rows(val_rows, upper_rows).astype(jnp.bfloat16)
    value_sum, proj_sum, table_sum = scatter_sums(value_part, proj_part, table_part)
    return (value_sum[None], proj_sum[None], table_sum[None])


def solution(mesh):
    return jax.shard_map(
        per_device,
        mesh=mesh,
        in_specs=(
            P(None, "dp", None),
            P(None, "dp", None),
            P(),
            P(),
            P(),
            P("section", None, None),
            P("section", None, None),
            P("section", None, None),
        ),
        out_specs=(P("section", "dp", None), P("section", "dp", None), P("section", None, "dp")),
        check_vma=False,
    )
```

```python
import functools
import math

import jax
import jax.numpy as jnp
from jax import lax
from jax.experimental import pallas as pl
from jax.experimental.pallas import tpu as pltpu
from jax.sharding import PartitionSpec as P

NORM_FLOOR = 0.1


def shifted(value, axis, steps):
    count = lax.axis_size(axis)
    leading, last = (max(0, -steps), min(count, count - steps))
    return lax.ppermute(value, axis, [(source, source + steps) for source in range(leading, last)])


def normalize(hidden):
    centre = jnp.mean(hidden, axis=-1, keepdims=True)
    centred = hidden - centre
    spread = jnp.mean(centred * centred, axis=-1, keepdims=True)
    inverse = lax.rsqrt(spread + NORM_FLOOR)
    return (centred * inverse, inverse)


def conditions(guide_bin, time_step, guide_table):
    total = guide_table.shape[1]
    half = total // 2
    frequency = jnp.exp(-math.log(10000.0) * jnp.arange(half, dtype=jnp.float32) / half)
    angle = time_step.astype(jnp.float32)[..., None] * frequency
    waves = jnp.concatenate([jnp.sin(angle), jnp.cos(angle)], axis=-1)
    bin_count = guide_table.shape[0]
    onehot = (guide_bin[..., None] == jnp.arange(bin_count, dtype=jnp.int32)).astype(jnp.float32)
    picked = jnp.einsum(
        "msb,bw->msw", onehot, guide_table.astype(jnp.float32), precision=lax.Precision.HIGHEST
    )
    return picked + 0.5 * waves


def contract_rows(left, right):
    return lax.dot_general(
        left, right, (((0,), (0,)), ((), ())), preferred_element_type=jnp.float32
    )


def forward_block(block_in, modulation, value_weight, proj_weight):
    width = block_in.shape[1]
    hidden = block_in.astype(jnp.float32)
    normed, inverse = normalize(hidden)
    shift = modulation[:, :width]
    scale = modulation[:, width : 2 * width]
    gate = modulation[:, 2 * width :]
    modulated = (normed * (1.0 + scale) + shift).astype(jnp.bfloat16)
    values = jnp.dot(modulated, value_weight, preferred_element_type=jnp.float32).astype(
        jnp.bfloat16
    )
    projected = jnp.dot(values, proj_weight, preferred_element_type=jnp.float32)
    block_out = (hidden + gate * projected).astype(jnp.bfloat16)
    return (block_out, modulated, values, projected)


def backward_block(block_in, projected, upstream, modulation, value_weight, proj_weight):
    width = block_in.shape[1]
    hidden = block_in.astype(jnp.float32)
    normed, inverse = normalize(hidden)
    scale = modulation[:, width : 2 * width]
    gate = modulation[:, 2 * width :]
    grad_up = upstream.astype(jnp.float32)
    grad_proj = (gate * grad_up).astype(jnp.bfloat16)
    grad_values = lax.dot_general(
        grad_proj, proj_weight, (((1,), (1,)), ((), ())), preferred_element_type=jnp.float32
    ).astype(jnp.bfloat16)
    grad_mod = lax.dot_general(
        grad_values, value_weight, (((1,), (1,)), ((), ())), preferred_element_type=jnp.float32
    )
    part_table = jnp.stack(
        [
            jnp.sum(grad_mod, axis=0),
            jnp.sum(grad_mod * normed, axis=0),
            jnp.sum(grad_up * projected, axis=0),
        ]
    )
    grad_norm = grad_mod * (1.0 + scale)
    centre_grad = jnp.mean(grad_norm, axis=-1, keepdims=True)
    cross = jnp.mean(grad_norm * normed, axis=-1, keepdims=True)
    grad_in = grad_up + inverse * (grad_norm - centre_grad - normed * cross)
    return (grad_in.astype(jnp.bfloat16), grad_values, grad_proj, part_table)


def per_device_scan(
    inputs, out_grad, guide_bin, time_step, guide_table, section_table, value_weight, proj_weight
):
    sections = lax.axis_size("section")
    section_id = lax.axis_index("section")
    position = lax.axis_index("dp")
    group_size = lax.axis_size("dp")
    tok_dev = inputs.shape[1]
    width = inputs.shape[2]
    value_width = value_weight.shape[2]
    batches = inputs.shape[0]
    samples = guide_bin.shape[1]
    tokens = tok_dev * group_size
    rows_per = tokens // samples
    parts = 1
    unit_rows = tok_dev // parts
    units = batches * parts
    condition = conditions(guide_bin, time_step, guide_table)
    weights_value = value_weight[0]
    weights_proj = proj_weight[0]
    section_row = section_table[0].reshape(-1)
    sample_ids = jnp.arange(samples, dtype=jnp.int32)

    def unit_modulation(unit_id):
        batch_id = unit_id // parts
        piece_id = unit_id % parts
        chosen = lax.dynamic_index_in_dim(condition, batch_id, 0, keepdims=False)
        global_rows = (
            position * tok_dev + piece_id * unit_rows + jnp.arange(unit_rows, dtype=jnp.int32)
        )
        owner = global_rows // rows_per
        onehot = (owner[:, None] == sample_ids[None, :]).astype(jnp.float32)
        picked = jnp.dot(
            onehot, chosen, precision=lax.Precision.HIGHEST, preferred_element_type=jnp.float32
        )
        return picked + section_row

    slots = units + 1
    keep_in = jnp.zeros((slots, unit_rows, width), jnp.bfloat16)
    keep_mod = jnp.zeros((slots, unit_rows, width), jnp.bfloat16)
    keep_val = jnp.zeros((slots, unit_rows, value_width), jnp.bfloat16)
    keep_proj = jnp.zeros((slots, unit_rows, width), jnp.float32)
    arriving = jnp.zeros((unit_rows, width), jnp.bfloat16)

    def forward_tick(carry, tick_id):
        incoming, saved_in, saved_mod, saved_val, saved_proj = carry
        unit_id = tick_id - section_id
        valid = (unit_id >= 0) & (unit_id < units)
        clipped = jnp.clip(unit_id, 0, units - 1)
        first = lax.dynamic_index_in_dim(inputs, clipped, 0, keepdims=False)
        block_in = jnp.where(section_id == 0, first, incoming)

        def forward_active(operand):
            return forward_block(operand, unit_modulation(clipped), weights_value, weights_proj)

        def forward_resting(operand):
            return (
                jnp.zeros_like(operand),
                jnp.zeros_like(operand),
                jnp.zeros((unit_rows, value_width), jnp.bfloat16),
                jnp.zeros((unit_rows, width), jnp.float32),
            )

        block_out, modulated, values, projected = lax.cond(
            valid, forward_active, forward_resting, block_in
        )
        slot_id = jnp.where(valid, unit_id, units)
        saved_in = lax.dynamic_update_index_in_dim(saved_in, block_in, slot_id, 0)
        saved_mod = lax.dynamic_update_index_in_dim(saved_mod, modulated, slot_id, 0)
        saved_val = lax.dynamic_update_index_in_dim(saved_val, values, slot_id, 0)
        saved_proj = lax.dynamic_update_index_in_dim(saved_proj, projected, slot_id, 0)
        sent = shifted(block_out, "section", 1)
        return ((sent, saved_in, saved_mod, saved_val, saved_proj), None)

    ticks = jnp.arange(units + sections - 1, dtype=jnp.int32)
    carry, unused = lax.scan(
        forward_tick, (arriving, keep_in, keep_mod, keep_val, keep_proj), ticks
    )
    arriving, keep_in, keep_mod, keep_val, keep_proj = carry
    store = jnp.zeros((slots, unit_rows, value_width), jnp.bfloat16)
    extra_zero = jnp.zeros((unit_rows, value_width), jnp.bfloat16)
    keep_grad = jnp.zeros((slots, unit_rows, width), jnp.bfloat16)
    proj_sum = jnp.zeros((value_width, width), jnp.float32)
    table_sum = jnp.zeros((3, width), jnp.float32)

    def backward_tick(carry, tick_id):
        incoming, store_now, grads_now, proj_now, table_now = carry
        unit_id = tick_id - (sections - 1 - section_id)
        valid = (unit_id >= 0) & (unit_id < units)
        clipped = jnp.clip(unit_id, 0, units - 1)
        last = lax.dynamic_index_in_dim(out_grad, clipped, 0, keepdims=False)
        upstream = jnp.where(section_id == sections - 1, last, incoming)
        block_in = lax.dynamic_index_in_dim(keep_in, clipped, 0, keepdims=False)
        modulated = lax.dynamic_index_in_dim(keep_mod, clipped, 0, keepdims=False)
        values = lax.dynamic_index_in_dim(keep_val, clipped, 0, keepdims=False)
        projected = lax.dynamic_index_in_dim(keep_proj, clipped, 0, keepdims=False)

        def backward_active(operand):
            grad_in, grad_values, grad_proj, part_table = backward_block(
                block_in, projected, operand, unit_modulation(clipped), weights_value, weights_proj
            )
            part_proj = jnp.zeros((value_width, width), jnp.float32)
            return (grad_in, grad_values, grad_proj, part_proj, part_table)

        def backward_resting(operand):
            return (
                jnp.zeros_like(operand),
                extra_zero,
                jnp.zeros((unit_rows, width), jnp.bfloat16),
                jnp.zeros((value_width, width), jnp.float32),
                jnp.zeros((3, width), jnp.float32),
            )

        grad_in, extra, grad_proj, part_proj, part_table = lax.cond(
            valid, backward_active, backward_resting, upstream
        )
        slot_id = jnp.where(valid, unit_id, units)
        store_now = lax.dynamic_update_index_in_dim(store_now, extra, slot_id, 0)
        grads_now = lax.dynamic_update_index_in_dim(grads_now, grad_proj, slot_id, 0)
        sent = shifted(grad_in, "section", -1)
        return ((sent, store_now, grads_now, proj_now + part_proj, table_now + part_table), None)

    carry, unused = lax.scan(
        backward_tick, (arriving, store, keep_grad, proj_sum, table_sum), ticks
    )
    arriving, store, keep_grad, proj_sum, table_sum = carry
    mod_rows = keep_mod[:units].reshape(units * unit_rows, width)
    grad_rows = store[:units].reshape(units * unit_rows, value_width)
    columns = mod_rows
    value_part = lax.psum_scatter(
        contract_rows(columns, grad_rows), "dp", scatter_dimension=0, tiled=True
    )
    val_rows = keep_val[:units].reshape(units * unit_rows, value_width)
    upper_rows = keep_grad[:units].reshape(units * unit_rows, width)
    columns = val_rows
    proj_part = lax.psum_scatter(
        contract_rows(columns, upper_rows), "dp", scatter_dimension=0, tiled=True
    )
    table_part = lax.psum_scatter(table_sum, "dp", scatter_dimension=1, tiled=True)
    return (value_part[None], proj_part[None], table_part[None])


MESH = pl.DeviceIdType.MESH


def scatter_kernel(far, value_ref, proj_ref, table_ref, value_out, proj_out, table_out,
                   core_in, own, side_out, side_in, far_out, far_in, table_in,
                   core_send, core_recv, side_send, side_recv, far_send, far_recv,
                   table_send, table_recv):
    group = 4 * far
    me = lax.axis_index("dp")
    core, side, place = me % 2, (me // 2) % 2, me // 4
    barrier = pltpu.get_barrier_semaphore()
    for step in range(1, group):
        pl.semaphore_signal(
            barrier, inc=1, device_id={"dp": (me + step) % group}, device_id_type=MESH
        )
    pl.semaphore_wait(barrier, group - 1)

    matrices = (proj_ref, value_ref)
    offsets = [(far // 2 + step) % far for step in range(far)]
    offsets = [offset for offset in offsets if offset] + [0]
    pieces = [(matrix, slot) for matrix in range(2) for slot in range(far)]

    def row(slot, which_side, which_core):
        return (((place + offsets[slot]) % far) * 2 + which_side) * 2 + which_core

    core_copies = {}
    for turn in range(2):
        for index, (matrix, slot) in enumerate(pieces):
            which = (1 - side) if turn == 0 else side
            copy = pltpu.make_async_remote_copy(
                src_ref=matrices[matrix].at[row(slot, which, 1 - core)],
                dst_ref=core_in.at[turn, index],
                send_sem=core_send.at[turn, index],
                recv_sem=core_recv.at[turn, index],
                device_id={"dp": me - core + (1 - core)},
                device_id_type=MESH,
            )
            copy.start()
            core_copies[turn, index] = copy
    table_copies = []
    for step in range(1, group):
        copy = pltpu.make_async_remote_copy(
            src_ref=table_ref.at[(me + step) % group],
            dst_ref=table_in.at[step - 1],
            send_sem=table_send.at[step - 1],
            recv_sem=table_recv.at[step - 1],
            device_id={"dp": (me + step) % group},
            device_id_type=MESH,
        )
        copy.start()
        table_copies.append(copy)

    side_copies = []
    for index, (matrix, slot) in enumerate(pieces):
        core_copies[0, index].wait_recv()
        mine = matrices[matrix][row(slot, 1 - side, core)].astype(jnp.float32)
        side_out[index] = (mine + core_in[0, index].astype(jnp.float32)).astype(jnp.bfloat16)
        copy = pltpu.make_async_remote_copy(
            src_ref=side_out.at[index],
            dst_ref=side_in.at[index],
            send_sem=side_send.at[index],
            recv_sem=side_recv.at[index],
            device_id={"dp": me + 2 - 4 * side},
            device_id_type=MESH,
        )
        copy.start()
        side_copies.append(copy)
    far_copies = {}
    for index, (matrix, slot) in enumerate(pieces):
        core_copies[1, index].wait_recv()
        mine = matrices[matrix][row(slot, side, core)].astype(jnp.float32)
        mine = mine + core_in[1, index].astype(jnp.float32)
        side_copies[index].wait_recv()
        mine = mine + side_in[index].astype(jnp.float32)
        if offsets[slot] == 0:
            own[matrix] = mine
        else:
            far_out[index] = mine.astype(jnp.bfloat16)
            copy = pltpu.make_async_remote_copy(
                src_ref=far_out.at[index],
                dst_ref=far_in.at[index],
                send_sem=far_send.at[index],
                recv_sem=far_recv.at[index],
                device_id={"dp": (me + 4 * offsets[slot]) % group},
                device_id_type=MESH,
            )
            copy.start()
            far_copies[index] = copy
    total = table_ref[me]
    for step in range(1, group):
        table_copies[step - 1].wait_recv()
        total = total + table_in[step - 1]
    table_out[...] = total
    for matrix, out in enumerate((proj_out, value_out)):
        result = own[matrix]
        for index, (which, slot) in enumerate(pieces):
            if which == matrix and index in far_copies:
                far_copies[index].wait_recv()
                result = result + far_in[index].astype(jnp.float32)
        out[...] = result
    for copy in list(core_copies.values()) + table_copies + side_copies:
        copy.wait_send()
    for copy in far_copies.values():
        copy.wait_send()


def scatter_sums(value_part, proj_part, table_part):
    group = lax.axis_size("dp")
    far = group // 4
    rows, width = value_part.shape[0] // group, value_part.shape[1]
    table_rows, lanes = table_part.shape[0], table_part.shape[1] // group
    tables = table_part.reshape(table_rows, group, lanes).transpose(1, 0, 2)
    tables = jnp.pad(tables, ((0, 0), (0, -table_rows % 8), (0, -lanes % 128)))
    count = 2 * far
    block = (rows, width)
    vmem = pl.BlockSpec(memory_space=pltpu.VMEM)
    dma = pltpu.SemaphoreType.DMA
    value_sum, proj_sum, table_sum = pl.pallas_call(
        functools.partial(scatter_kernel, far),
        out_shape=(
            jax.ShapeDtypeStruct(block, jnp.float32),
            jax.ShapeDtypeStruct((value_part.shape[0] // group, proj_part.shape[1]), jnp.float32),
            jax.ShapeDtypeStruct(tables.shape[1:], jnp.float32),
        ),
        in_specs=[vmem] * 3,
        out_specs=(vmem,) * 3,
        scratch_shapes=[
            pltpu.VMEM((2, count) + block, jnp.bfloat16),
            pltpu.VMEM((2,) + block, jnp.float32),
            pltpu.VMEM((count,) + block, jnp.bfloat16),
            pltpu.VMEM((count,) + block, jnp.bfloat16),
            pltpu.VMEM((count,) + block, jnp.bfloat16),
            pltpu.VMEM((count,) + block, jnp.bfloat16),
            pltpu.VMEM((group - 1,) + tables.shape[1:], jnp.float32),
            dma((2, count)), dma((2, count)), dma((count,)), dma((count,)),
            dma((count,)), dma((count,)), dma((group - 1,)), dma((group - 1,)),
        ],
        compiler_params=pltpu.CompilerParams(
            collective_id=0, has_side_effects=True, vmem_limit_bytes=56 * 1024 * 1024
        ),
    )(
        value_part.reshape((group,) + block),
        proj_part.reshape((group,) + block),
        tables,
    )
    return value_sum, proj_sum, table_sum[:table_rows, :lanes]


def modulation_rows(guide_bin, time_step, guide_table, section_row, tok_dev):
    group_size = lax.axis_size("dp")
    position = lax.axis_index("dp")
    batches, samples = guide_bin.shape
    rows_per = tok_dev * group_size // samples
    if rows_per % tok_dev == 0:
        owner = (position * tok_dev) // rows_per
        guide_bin = lax.dynamic_slice_in_dim(guide_bin, owner, 1, 1)
        time_step = lax.dynamic_slice_in_dim(time_step, owner, 1, 1)
    kept = guide_bin.shape[1]
    total = guide_table.shape[1]
    half = total // 2
    frequency = jnp.exp(-math.log(10000.0) * jnp.arange(half, dtype=jnp.float32) / half)
    angle = time_step.reshape(-1, 1).astype(jnp.float32) * frequency
    waves = jnp.concatenate([jnp.sin(angle), jnp.cos(angle)], axis=-1)
    bins = jnp.arange(guide_table.shape[0], dtype=jnp.int32)
    picked = jnp.sum(
        jnp.where(
            (guide_bin.reshape(-1, 1) == bins)[:, :, None], guide_table.astype(jnp.float32), 0.0
        ),
        axis=1,
    )
    rows = (picked + 0.5 * waves + section_row).reshape(batches, kept, total)
    if kept == samples and samples > 1:
        owners = (position * tok_dev + jnp.arange(tok_dev, dtype=jnp.int32)) // rows_per
        rows = jnp.take(rows, owners, axis=1)
    return rows


def blocks_kernel(x_ref, up_ref, mod_ref, wv_ref, wp_ref, mod_out, val_out, gv_out, gp_out,
                  tab_out, proj_s, gm_s, send_s, arrive_s, send_sem, recv_sem):
    units, rows, width = x_ref.shape
    depth = wv_ref.shape[1]
    chunk = math.gcd(rows, 16)
    section = lax.axis_index("section")
    barrier = pltpu.get_barrier_semaphore()
    pl.semaphore_signal(
        barrier, inc=1, device_id={"section": 1 - section}, device_id_type=MESH
    )
    pl.semaphore_wait(barrier, 1)
    tab_out[...] = jnp.zeros_like(tab_out)

    def hop(unit):
        return pltpu.make_async_remote_copy(
            src_ref=send_s.at[unit],
            dst_ref=arrive_s.at[unit],
            send_sem=send_sem.at[unit],
            recv_sem=recv_sem.at[unit],
            device_id={"section": 1 - section},
            device_id_type=MESH,
        )

    def each_chunk(body):
        @pl.loop(0, rows // chunk)
        def step(index):
            body(pl.ds(pl.multiple_of(index * chunk, chunk), chunk))

    def multiply(size, body):
        tile = math.gcd(size, 512)

        @pl.loop(0, size // tile)
        def step(index):
            body(pl.ds(pl.multiple_of(index * tile, tile), tile))

    def add_rows(place, value):
        tab_out[place] += jnp.sum(value.reshape(chunk // 8, 8, width), axis=0)

    def forward(unit, source, send):
        def modulate(part):
            normed, inverse = normalize(source[unit, part].astype(jnp.float32))
            scaled = normed * (1.0 + mod_ref[unit, 1:2]) + mod_ref[unit, 0:1]
            mod_out[unit, part] = scaled.astype(jnp.bfloat16)

        def first_dot(part):
            val_out[unit, :, part] = jnp.dot(
                mod_out[unit], wv_ref[:, part], preferred_element_type=jnp.float32
            ).astype(jnp.bfloat16)

        def second_dot(part):
            proj_s[unit, :, part] = jnp.dot(
                val_out[unit], wp_ref[:, part], preferred_element_type=jnp.float32
            )

        def add_gated(part):
            hidden = source[unit, part].astype(jnp.float32)
            block_out = hidden + mod_ref[unit, 2:3] * proj_s[unit, part]
            send_s[unit, part] = block_out.astype(jnp.bfloat16)

        each_chunk(modulate)
        multiply(depth, first_dot)
        multiply(width, second_dot)
        if send:
            each_chunk(add_gated)

    def backward(unit, source, upstream, send):
        def gated(part):
            grad_up = upstream[unit, part].astype(jnp.float32)
            gp_out[unit, part] = (mod_ref[unit, 2:3] * grad_up).astype(jnp.bfloat16)
            add_rows(2, grad_up * proj_s[unit, part])

        def first_dot(part):
            gv_out[unit, :, part] = lax.dot_general(
                gp_out[unit], wp_ref[part, :], (((1,), (1,)), ((), ())),
                preferred_element_type=jnp.float32,
            ).astype(jnp.bfloat16)

        def second_dot(part):
            gm_s[:, part] = lax.dot_general(
                gv_out[unit], wv_ref[part, :], (((1,), (1,)), ((), ())),
                preferred_element_type=jnp.float32,
            )

        def to_input(part):
            normed, inverse = normalize(source[unit, part].astype(jnp.float32))
            grad_mod = gm_s[part]
            add_rows(0, grad_mod)
            add_rows(1, grad_mod * normed)
            if send:
                grad_norm = grad_mod * (1.0 + mod_ref[unit, 1:2])
                centre_grad = jnp.mean(grad_norm, axis=-1, keepdims=True)
                cross = jnp.mean(grad_norm * normed, axis=-1, keepdims=True)
                grad_up = upstream[unit, part].astype(jnp.float32)
                grad_in = grad_up + inverse * (grad_norm - centre_grad - normed * cross)
                send_s[unit, part] = grad_in.astype(jnp.bfloat16)

        each_chunk(gated)
        multiply(depth, first_dot)
        multiply(width, second_dot)
        each_chunk(to_input)

    @pl.when(section == 0)
    def earlier():
        @pl.loop(0, units)
        def out(unit):
            forward(unit, x_ref, True)
            hop(unit).start()

        @pl.loop(0, units)
        def back(unit):
            hop(unit).wait_recv()
            backward(unit, x_ref, arrive_s, False)

    @pl.when(section == 1)
    def later():
        @pl.loop(0, units)
        def both(unit):
            hop(unit).wait_recv()
            forward(unit, arrive_s, False)
            backward(unit, arrive_s, up_ref, True)
            hop(unit).start()

    @pl.loop(0, units)
    def finish(unit):
        hop(unit).wait_send()


def per_device(
    inputs, out_grad, guide_bin, time_step, guide_table, section_table, value_weight, proj_weight
):
    units, rows, width = inputs.shape
    depth = value_weight.shape[2]
    group = lax.axis_size("dp")
    per_sample = rows * group // guide_bin.shape[1]
    if lax.axis_size("section") != 2 or group % 4 or per_sample % rows or rows % 8:
        return per_device_scan(
            inputs, out_grad, guide_bin, time_step, guide_table, section_table,
            value_weight, proj_weight,
        )
    modulation = modulation_rows(
        guide_bin, time_step, guide_table, section_table[0].reshape(-1), rows
    ).reshape(units, 3, width)
    vmem = pl.BlockSpec(memory_space=pltpu.VMEM)
    wide = jax.ShapeDtypeStruct((units, rows, width), jnp.bfloat16)
    deep = jax.ShapeDtypeStruct((units, rows, depth), jnp.bfloat16)
    modulated, values, grad_values, grad_proj, tables = pl.pallas_call(
        blocks_kernel,
        out_shape=(wide, deep, deep, wide, jax.ShapeDtypeStruct((3, 8, width), jnp.float32)),
        in_specs=[vmem] * 5,
        out_specs=(vmem,) * 5,
        scratch_shapes=[
            pltpu.VMEM((units, rows, width), jnp.float32),
            pltpu.VMEM((rows, width), jnp.float32),
            pltpu.VMEM((units, rows, width), jnp.bfloat16),
            pltpu.VMEM((units, rows, width), jnp.bfloat16),
            pltpu.SemaphoreType.DMA((units,)),
            pltpu.SemaphoreType.DMA((units,)),
        ],
        compiler_params=pltpu.CompilerParams(
            collective_id=1, has_side_effects=True, vmem_limit_bytes=56 * 1024 * 1024
        ),
    )(inputs, out_grad, modulation, value_weight[0], proj_weight[0])
    count = units * rows
    value_part = contract_rows(
        modulated.reshape(count, width), grad_values.reshape(count, depth)
    ).astype(jnp.bfloat16)
    proj_part = contract_rows(
        values.reshape(count, depth), grad_proj.reshape(count, width)
    ).astype(jnp.bfloat16)
    value_sum, proj_sum, table_sum = scatter_sums(value_part, proj_part, jnp.sum(tables, axis=1))
    return (value_sum[None], proj_sum[None], table_sum[None])


def solution(mesh):
    return jax.shard_map(
        per_device,
        mesh=mesh,
        in_specs=(
            P(None, "dp", None),
            P(None, "dp", None),
            P(),
            P(),
            P(),
            P("section", None, None),
            P("section", None, None),
            P("section", None, None),
        ),
        out_specs=(P("section", "dp", None), P("section", "dp", None), P("section", None, "dp")),
        check_vma=False,
    )
```

```python
import functools
import math

import jax
import jax.numpy as jnp
from jax import lax
from jax.experimental import pallas as pl
from jax.experimental.pallas import tpu as pltpu
from jax.sharding import PartitionSpec as P

NORM_FLOOR = 0.1


def shifted(value, axis, steps):
    count = lax.axis_size(axis)
    leading, last = (max(0, -steps), min(count, count - steps))
    return lax.ppermute(value, axis, [(source, source + steps) for source in range(leading, last)])


def normalize(hidden):
    centre = jnp.mean(hidden, axis=-1, keepdims=True)
    centred = hidden - centre
    spread = jnp.mean(centred * centred, axis=-1, keepdims=True)
    inverse = lax.rsqrt(spread + NORM_FLOOR)
    return (centred * inverse, inverse)


def conditions(guide_bin, time_step, guide_table):
    total = guide_table.shape[1]
    half = total // 2
    frequency = jnp.exp(-math.log(10000.0) * jnp.arange(half, dtype=jnp.float32) / half)
    angle = time_step.astype(jnp.float32)[..., None] * frequency
    waves = jnp.concatenate([jnp.sin(angle), jnp.cos(angle)], axis=-1)
    bin_count = guide_table.shape[0]
    onehot = (guide_bin[..., None] == jnp.arange(bin_count, dtype=jnp.int32)).astype(jnp.float32)
    picked = jnp.einsum(
        "msb,bw->msw", onehot, guide_table.astype(jnp.float32), precision=lax.Precision.HIGHEST
    )
    return picked + 0.5 * waves


def contract_rows(left, right):
    return lax.dot_general(
        left, right, (((0,), (0,)), ((), ())), preferred_element_type=jnp.float32
    )


def forward_block(block_in, modulation, value_weight, proj_weight):
    width = block_in.shape[1]
    hidden = block_in.astype(jnp.float32)
    normed, inverse = normalize(hidden)
    shift = modulation[:, :width]
    scale = modulation[:, width : 2 * width]
    gate = modulation[:, 2 * width :]
    modulated = (normed * (1.0 + scale) + shift).astype(jnp.bfloat16)
    values = jnp.dot(modulated, value_weight, preferred_element_type=jnp.float32).astype(
        jnp.bfloat16
    )
    projected = jnp.dot(values, proj_weight, preferred_element_type=jnp.float32)
    block_out = (hidden + gate * projected).astype(jnp.bfloat16)
    return (block_out, modulated, values, projected)


def backward_block(block_in, projected, upstream, modulation, value_weight, proj_weight):
    width = block_in.shape[1]
    hidden = block_in.astype(jnp.float32)
    normed, inverse = normalize(hidden)
    scale = modulation[:, width : 2 * width]
    gate = modulation[:, 2 * width :]
    grad_up = upstream.astype(jnp.float32)
    grad_proj = (gate * grad_up).astype(jnp.bfloat16)
    grad_values = lax.dot_general(
        grad_proj, proj_weight, (((1,), (1,)), ((), ())), preferred_element_type=jnp.float32
    ).astype(jnp.bfloat16)
    grad_mod = lax.dot_general(
        grad_values, value_weight, (((1,), (1,)), ((), ())), preferred_element_type=jnp.float32
    )
    part_table = jnp.stack(
        [
            jnp.sum(grad_mod, axis=0),
            jnp.sum(grad_mod * normed, axis=0),
            jnp.sum(grad_up * projected, axis=0),
        ]
    )
    grad_norm = grad_mod * (1.0 + scale)
    centre_grad = jnp.mean(grad_norm, axis=-1, keepdims=True)
    cross = jnp.mean(grad_norm * normed, axis=-1, keepdims=True)
    grad_in = grad_up + inverse * (grad_norm - centre_grad - normed * cross)
    return (grad_in.astype(jnp.bfloat16), grad_values, grad_proj, part_table)


def per_device_scan(
    inputs, out_grad, guide_bin, time_step, guide_table, section_table, value_weight, proj_weight
):
    sections = lax.axis_size("section")
    section_id = lax.axis_index("section")
    position = lax.axis_index("dp")
    group_size = lax.axis_size("dp")
    tok_dev = inputs.shape[1]
    width = inputs.shape[2]
    value_width = value_weight.shape[2]
    batches = inputs.shape[0]
    samples = guide_bin.shape[1]
    tokens = tok_dev * group_size
    rows_per = tokens // samples
    parts = 1
    unit_rows = tok_dev // parts
    units = batches * parts
    condition = conditions(guide_bin, time_step, guide_table)
    weights_value = value_weight[0]
    weights_proj = proj_weight[0]
    section_row = section_table[0].reshape(-1)
    sample_ids = jnp.arange(samples, dtype=jnp.int32)

    def unit_modulation(unit_id):
        batch_id = unit_id // parts
        piece_id = unit_id % parts
        chosen = lax.dynamic_index_in_dim(condition, batch_id, 0, keepdims=False)
        global_rows = (
            position * tok_dev + piece_id * unit_rows + jnp.arange(unit_rows, dtype=jnp.int32)
        )
        owner = global_rows // rows_per
        onehot = (owner[:, None] == sample_ids[None, :]).astype(jnp.float32)
        picked = jnp.dot(
            onehot, chosen, precision=lax.Precision.HIGHEST, preferred_element_type=jnp.float32
        )
        return picked + section_row

    slots = units + 1
    keep_in = jnp.zeros((slots, unit_rows, width), jnp.bfloat16)
    keep_mod = jnp.zeros((slots, unit_rows, width), jnp.bfloat16)
    keep_val = jnp.zeros((slots, unit_rows, value_width), jnp.bfloat16)
    keep_proj = jnp.zeros((slots, unit_rows, width), jnp.float32)
    arriving = jnp.zeros((unit_rows, width), jnp.bfloat16)

    def forward_tick(carry, tick_id):
        incoming, saved_in, saved_mod, saved_val, saved_proj = carry
        unit_id = tick_id - section_id
        valid = (unit_id >= 0) & (unit_id < units)
        clipped = jnp.clip(unit_id, 0, units - 1)
        first = lax.dynamic_index_in_dim(inputs, clipped, 0, keepdims=False)
        block_in = jnp.where(section_id == 0, first, incoming)

        def forward_active(operand):
            return forward_block(operand, unit_modulation(clipped), weights_value, weights_proj)

        def forward_resting(operand):
            return (
                jnp.zeros_like(operand),
                jnp.zeros_like(operand),
                jnp.zeros((unit_rows, value_width), jnp.bfloat16),
                jnp.zeros((unit_rows, width), jnp.float32),
            )

        block_out, modulated, values, projected = lax.cond(
            valid, forward_active, forward_resting, block_in
        )
        slot_id = jnp.where(valid, unit_id, units)
        saved_in = lax.dynamic_update_index_in_dim(saved_in, block_in, slot_id, 0)
        saved_mod = lax.dynamic_update_index_in_dim(saved_mod, modulated, slot_id, 0)
        saved_val = lax.dynamic_update_index_in_dim(saved_val, values, slot_id, 0)
        saved_proj = lax.dynamic_update_index_in_dim(saved_proj, projected, slot_id, 0)
        sent = shifted(block_out, "section", 1)
        return ((sent, saved_in, saved_mod, saved_val, saved_proj), None)

    ticks = jnp.arange(units + sections - 1, dtype=jnp.int32)
    carry, unused = lax.scan(
        forward_tick, (arriving, keep_in, keep_mod, keep_val, keep_proj), ticks
    )
    arriving, keep_in, keep_mod, keep_val, keep_proj = carry
    store = jnp.zeros((slots, unit_rows, value_width), jnp.bfloat16)
    extra_zero = jnp.zeros((unit_rows, value_width), jnp.bfloat16)
    keep_grad = jnp.zeros((slots, unit_rows, width), jnp.bfloat16)
    proj_sum = jnp.zeros((value_width, width), jnp.float32)
    table_sum = jnp.zeros((3, width), jnp.float32)

    def backward_tick(carry, tick_id):
        incoming, store_now, grads_now, proj_now, table_now = carry
        unit_id = tick_id - (sections - 1 - section_id)
        valid = (unit_id >= 0) & (unit_id < units)
        clipped = jnp.clip(unit_id, 0, units - 1)
        last = lax.dynamic_index_in_dim(out_grad, clipped, 0, keepdims=False)
        upstream = jnp.where(section_id == sections - 1, last, incoming)
        block_in = lax.dynamic_index_in_dim(keep_in, clipped, 0, keepdims=False)
        modulated = lax.dynamic_index_in_dim(keep_mod, clipped, 0, keepdims=False)
        values = lax.dynamic_index_in_dim(keep_val, clipped, 0, keepdims=False)
        projected = lax.dynamic_index_in_dim(keep_proj, clipped, 0, keepdims=False)

        def backward_active(operand):
            grad_in, grad_values, grad_proj, part_table = backward_block(
                block_in, projected, operand, unit_modulation(clipped), weights_value, weights_proj
            )
            part_proj = jnp.zeros((value_width, width), jnp.float32)
            return (grad_in, grad_values, grad_proj, part_proj, part_table)

        def backward_resting(operand):
            return (
                jnp.zeros_like(operand),
                extra_zero,
                jnp.zeros((unit_rows, width), jnp.bfloat16),
                jnp.zeros((value_width, width), jnp.float32),
                jnp.zeros((3, width), jnp.float32),
            )

        grad_in, extra, grad_proj, part_proj, part_table = lax.cond(
            valid, backward_active, backward_resting, upstream
        )
        slot_id = jnp.where(valid, unit_id, units)
        store_now = lax.dynamic_update_index_in_dim(store_now, extra, slot_id, 0)
        grads_now = lax.dynamic_update_index_in_dim(grads_now, grad_proj, slot_id, 0)
        sent = shifted(grad_in, "section", -1)
        return ((sent, store_now, grads_now, proj_now + part_proj, table_now + part_table), None)

    carry, unused = lax.scan(
        backward_tick, (arriving, store, keep_grad, proj_sum, table_sum), ticks
    )
    arriving, store, keep_grad, proj_sum, table_sum = carry
    mod_rows = keep_mod[:units].reshape(units * unit_rows, width)
    grad_rows = store[:units].reshape(units * unit_rows, value_width)
    columns = mod_rows
    value_part = lax.psum_scatter(
        contract_rows(columns, grad_rows), "dp", scatter_dimension=0, tiled=True
    )
    val_rows = keep_val[:units].reshape(units * unit_rows, value_width)
    upper_rows = keep_grad[:units].reshape(units * unit_rows, width)
    columns = val_rows
    proj_part = lax.psum_scatter(
        contract_rows(columns, upper_rows), "dp", scatter_dimension=0, tiled=True
    )
    table_part = lax.psum_scatter(table_sum, "dp", scatter_dimension=1, tiled=True)
    return (value_part[None], proj_part[None], table_part[None])


MESH = pl.DeviceIdType.MESH


def scatter_kernel(far, value_ref, proj_ref, table_ref, value_out, proj_out, table_out,
                   core_in, own, side_out, side_in, far_out, far_in, table_in,
                   core_send, core_recv, side_send, side_recv, far_send, far_recv,
                   table_send, table_recv):
    group = 4 * far
    me = lax.axis_index("dp")
    core, side, place = me % 2, (me // 2) % 2, me // 4
    barrier = pltpu.get_barrier_semaphore()
    for step in range(1, group):
        pl.semaphore_signal(
            barrier, inc=1, device_id={"dp": (me + step) % group}, device_id_type=MESH
        )
    pl.semaphore_wait(barrier, group - 1)

    matrices = (proj_ref, value_ref)
    offsets = [(far // 2 + step) % far for step in range(far)]
    offsets = [offset for offset in offsets if offset] + [0]
    pieces = [(matrix, slot) for matrix in range(2) for slot in range(far)]

    def row(slot, which_side, which_core):
        return (((place + offsets[slot]) % far) * 2 + which_side) * 2 + which_core

    core_copies = {}
    for turn in range(2):
        for index, (matrix, slot) in enumerate(pieces):
            which = (1 - side) if turn == 0 else side
            copy = pltpu.make_async_remote_copy(
                src_ref=matrices[matrix].at[row(slot, which, 1 - core)],
                dst_ref=core_in.at[turn, index],
                send_sem=core_send.at[turn, index],
                recv_sem=core_recv.at[turn, index],
                device_id={"dp": me - core + (1 - core)},
                device_id_type=MESH,
            )
            copy.start()
            core_copies[turn, index] = copy
    table_copies = []
    for step in range(1, group):
        copy = pltpu.make_async_remote_copy(
            src_ref=table_ref.at[(me + step) % group],
            dst_ref=table_in.at[step - 1],
            send_sem=table_send.at[step - 1],
            recv_sem=table_recv.at[step - 1],
            device_id={"dp": (me + step) % group},
            device_id_type=MESH,
        )
        copy.start()
        table_copies.append(copy)

    side_copies = []
    for index, (matrix, slot) in enumerate(pieces):
        core_copies[0, index].wait_recv()
        mine = matrices[matrix][row(slot, 1 - side, core)].astype(jnp.float32)
        side_out[index] = (mine + core_in[0, index].astype(jnp.float32)).astype(jnp.bfloat16)
        copy = pltpu.make_async_remote_copy(
            src_ref=side_out.at[index],
            dst_ref=side_in.at[index],
            send_sem=side_send.at[index],
            recv_sem=side_recv.at[index],
            device_id={"dp": me + 2 - 4 * side},
            device_id_type=MESH,
        )
        copy.start()
        side_copies.append(copy)
    far_copies = {}
    for index, (matrix, slot) in enumerate(pieces):
        core_copies[1, index].wait_recv()
        mine = matrices[matrix][row(slot, side, core)].astype(jnp.float32)
        mine = mine + core_in[1, index].astype(jnp.float32)
        side_copies[index].wait_recv()
        mine = mine + side_in[index].astype(jnp.float32)
        if offsets[slot] == 0:
            own[matrix] = mine
        else:
            far_out[index] = mine.astype(jnp.bfloat16)
            copy = pltpu.make_async_remote_copy(
                src_ref=far_out.at[index],
                dst_ref=far_in.at[index],
                send_sem=far_send.at[index],
                recv_sem=far_recv.at[index],
                device_id={"dp": (me + 4 * offsets[slot]) % group},
                device_id_type=MESH,
            )
            copy.start()
            far_copies[index] = copy
    total = table_ref[me]
    for step in range(1, group):
        table_copies[step - 1].wait_recv()
        total = total + table_in[step - 1]
    table_out[...] = total
    for matrix, out in enumerate((proj_out, value_out)):
        result = own[matrix]
        for index, (which, slot) in enumerate(pieces):
            if which == matrix and index in far_copies:
                far_copies[index].wait_recv()
                result = result + far_in[index].astype(jnp.float32)
        out[...] = result
    for copy in list(core_copies.values()) + table_copies + side_copies:
        copy.wait_send()
    for copy in far_copies.values():
        copy.wait_send()


def scatter_sums(value_part, proj_part, table_part):
    group = lax.axis_size("dp")
    far = group // 4
    rows, width = value_part.shape[0] // group, value_part.shape[1]
    table_rows, lanes = table_part.shape[0], table_part.shape[1] // group
    tables = table_part.reshape(table_rows, group, lanes).transpose(1, 0, 2)
    tables = jnp.pad(tables, ((0, 0), (0, -table_rows % 8), (0, -lanes % 128)))
    count = 2 * far
    block = (rows, width)
    vmem = pl.BlockSpec(memory_space=pltpu.VMEM)
    dma = pltpu.SemaphoreType.DMA
    value_sum, proj_sum, table_sum = pl.pallas_call(
        functools.partial(scatter_kernel, far),
        out_shape=(
            jax.ShapeDtypeStruct(block, jnp.float32),
            jax.ShapeDtypeStruct((value_part.shape[0] // group, proj_part.shape[1]), jnp.float32),
            jax.ShapeDtypeStruct(tables.shape[1:], jnp.float32),
        ),
        in_specs=[vmem] * 3,
        out_specs=(vmem,) * 3,
        scratch_shapes=[
            pltpu.VMEM((2, count) + block, jnp.bfloat16),
            pltpu.VMEM((2,) + block, jnp.float32),
            pltpu.VMEM((count,) + block, jnp.bfloat16),
            pltpu.VMEM((count,) + block, jnp.bfloat16),
            pltpu.VMEM((count,) + block, jnp.bfloat16),
            pltpu.VMEM((count,) + block, jnp.bfloat16),
            pltpu.VMEM((group - 1,) + tables.shape[1:], jnp.float32),
            dma((2, count)), dma((2, count)), dma((count,)), dma((count,)),
            dma((count,)), dma((count,)), dma((group - 1,)), dma((group - 1,)),
        ],
        compiler_params=pltpu.CompilerParams(
            collective_id=0, has_side_effects=True, vmem_limit_bytes=56 * 1024 * 1024
        ),
    )(
        value_part.reshape((group,) + block),
        proj_part.reshape((group,) + block),
        tables,
    )
    return value_sum, proj_sum, table_sum[:table_rows, :lanes]


def modulation_rows(guide_bin, time_step, guide_table, section_row, tok_dev):
    group_size = lax.axis_size("dp")
    position = lax.axis_index("dp")
    batches, samples = guide_bin.shape
    rows_per = tok_dev * group_size // samples
    if rows_per % tok_dev == 0:
        owner = (position * tok_dev) // rows_per
        guide_bin = lax.dynamic_slice_in_dim(guide_bin, owner, 1, 1)
        time_step = lax.dynamic_slice_in_dim(time_step, owner, 1, 1)
    kept = guide_bin.shape[1]
    total = guide_table.shape[1]
    half = total // 2
    frequency = jnp.exp(-math.log(10000.0) * jnp.arange(half, dtype=jnp.float32) / half)
    angle = time_step.reshape(-1, 1).astype(jnp.float32) * frequency
    waves = jnp.concatenate([jnp.sin(angle), jnp.cos(angle)], axis=-1)
    bins = jnp.arange(guide_table.shape[0], dtype=jnp.int32)
    picked = jnp.sum(
        jnp.where(
            (guide_bin.reshape(-1, 1) == bins)[:, :, None], guide_table.astype(jnp.float32), 0.0
        ),
        axis=1,
    )
    rows = (picked + 0.5 * waves + section_row).reshape(batches, kept, total)
    if kept == samples and samples > 1:
        owners = (position * tok_dev + jnp.arange(tok_dev, dtype=jnp.int32)) // rows_per
        rows = jnp.take(rows, owners, axis=1)
    return rows


def blocks_kernel(x_ref, up_ref, mod_ref, wv_ref, wp_ref, mod_out, val_out, gv_out, gp_out,
                  tab_out, proj_s, gm_s, send_s, arrive_s, send_sem, recv_sem):
    units, rows, width = x_ref.shape
    depth = wv_ref.shape[1]
    chunk = math.gcd(rows, 32)
    section = lax.axis_index("section")
    barrier = pltpu.get_barrier_semaphore()
    pl.semaphore_signal(
        barrier, inc=1, device_id={"section": 1 - section}, device_id_type=MESH
    )
    pl.semaphore_wait(barrier, 1)
    tab_out[...] = jnp.zeros_like(tab_out)

    def hop(unit):
        return pltpu.make_async_remote_copy(
            src_ref=send_s.at[unit],
            dst_ref=arrive_s.at[unit],
            send_sem=send_sem.at[unit],
            recv_sem=recv_sem.at[unit],
            device_id={"section": 1 - section},
            device_id_type=MESH,
        )

    def each_chunk(body):
        @pl.loop(0, rows // chunk)
        def step(index):
            body(pl.ds(pl.multiple_of(index * chunk, chunk), chunk))

    def multiply(size, body):
        tile = math.gcd(size, 512)

        @pl.loop(0, size // tile)
        def step(index):
            body(pl.ds(pl.multiple_of(index * tile, tile), tile))

    def add_rows(place, value):
        tab_out[place] += jnp.sum(value.reshape(chunk // 8, 8, width), axis=0)

    def forward(unit, source, send):
        def modulate(part):
            normed, inverse = normalize(source[unit, part].astype(jnp.float32))
            scaled = normed * (1.0 + mod_ref[unit, 1:2]) + mod_ref[unit, 0:1]
            mod_out[unit, part] = scaled.astype(jnp.bfloat16)

        def first_dot(part):
            val_out[unit, :, part] = jnp.dot(
                mod_out[unit], wv_ref[:, part], preferred_element_type=jnp.float32
            ).astype(jnp.bfloat16)

        def second_dot(part):
            proj_s[unit, :, part] = jnp.dot(
                val_out[unit], wp_ref[:, part], preferred_element_type=jnp.float32
            )

        def add_gated(part):
            hidden = source[unit, part].astype(jnp.float32)
            block_out = hidden + mod_ref[unit, 2:3] * proj_s[unit, part]
            send_s[unit, part] = block_out.astype(jnp.bfloat16)

        each_chunk(modulate)
        multiply(depth, first_dot)
        multiply(width, second_dot)
        if send:
            each_chunk(add_gated)

    def backward(unit, source, upstream, send):
        def gated(part):
            grad_up = upstream[unit, part].astype(jnp.float32)
            gp_out[unit, part] = (mod_ref[unit, 2:3] * grad_up).astype(jnp.bfloat16)
            add_rows(2, grad_up * proj_s[unit, part])

        def first_dot(part):
            gv_out[unit, :, part] = lax.dot_general(
                gp_out[unit], wp_ref[part, :], (((1,), (1,)), ((), ())),
                preferred_element_type=jnp.float32,
            ).astype(jnp.bfloat16)

        def second_dot(part):
            gm_s[:, part] = lax.dot_general(
                gv_out[unit], wv_ref[part, :], (((1,), (1,)), ((), ())),
                preferred_element_type=jnp.float32,
            )

        def to_input(part):
            normed, inverse = normalize(source[unit, part].astype(jnp.float32))
            grad_mod = gm_s[part]
            add_rows(0, grad_mod)
            add_rows(1, grad_mod * normed)
            if send:
                grad_norm = grad_mod * (1.0 + mod_ref[unit, 1:2])
                centre_grad = jnp.mean(grad_norm, axis=-1, keepdims=True)
                cross = jnp.mean(grad_norm * normed, axis=-1, keepdims=True)
                grad_up = upstream[unit, part].astype(jnp.float32)
                grad_in = grad_up + inverse * (grad_norm - centre_grad - normed * cross)
                send_s[unit, part] = grad_in.astype(jnp.bfloat16)

        each_chunk(gated)
        multiply(depth, first_dot)
        multiply(width, second_dot)
        each_chunk(to_input)

    @pl.when(section == 0)
    def earlier():
        @pl.loop(0, units)
        def out(unit):
            forward(unit, x_ref, True)
            hop(unit).start()

        @pl.loop(0, units)
        def back(unit):
            hop(unit).wait_recv()
            backward(unit, x_ref, arrive_s, False)

    @pl.when(section == 1)
    def later():
        @pl.loop(0, units)
        def both(unit):
            hop(unit).wait_recv()
            forward(unit, arrive_s, False)
            backward(unit, arrive_s, up_ref, True)
            hop(unit).start()

    @pl.loop(0, units)
    def finish(unit):
        hop(unit).wait_send()


def per_device(
    inputs, out_grad, guide_bin, time_step, guide_table, section_table, value_weight, proj_weight
):
    units, rows, width = inputs.shape
    depth = value_weight.shape[2]
    group = lax.axis_size("dp")
    per_sample = rows * group // guide_bin.shape[1]
    if lax.axis_size("section") != 2 or group % 4 or per_sample % rows or rows % 8:
        return per_device_scan(
            inputs, out_grad, guide_bin, time_step, guide_table, section_table,
            value_weight, proj_weight,
        )
    modulation = modulation_rows(
        guide_bin, time_step, guide_table, section_table[0].reshape(-1), rows
    ).reshape(units, 3, width)
    vmem = pl.BlockSpec(memory_space=pltpu.VMEM)
    wide = jax.ShapeDtypeStruct((units, rows, width), jnp.bfloat16)
    deep = jax.ShapeDtypeStruct((units, rows, depth), jnp.bfloat16)
    modulated, values, grad_values, grad_proj, tables = pl.pallas_call(
        blocks_kernel,
        out_shape=(wide, deep, deep, wide, jax.ShapeDtypeStruct((3, 8, width), jnp.float32)),
        in_specs=[vmem] * 5,
        out_specs=(vmem,) * 5,
        scratch_shapes=[
            pltpu.VMEM((units, rows, width), jnp.float32),
            pltpu.VMEM((rows, width), jnp.float32),
            pltpu.VMEM((units, rows, width), jnp.bfloat16),
            pltpu.VMEM((units, rows, width), jnp.bfloat16),
            pltpu.SemaphoreType.DMA((units,)),
            pltpu.SemaphoreType.DMA((units,)),
        ],
        compiler_params=pltpu.CompilerParams(
            collective_id=1, has_side_effects=True, vmem_limit_bytes=56 * 1024 * 1024
        ),
    )(inputs, out_grad, modulation, value_weight[0], proj_weight[0])
    count = units * rows
    value_part = contract_rows(
        modulated.reshape(count, width), grad_values.reshape(count, depth)
    ).astype(jnp.bfloat16)
    proj_part = contract_rows(
        values.reshape(count, depth), grad_proj.reshape(count, width)
    ).astype(jnp.bfloat16)
    value_sum, proj_sum, table_sum = scatter_sums(value_part, proj_part, jnp.sum(tables, axis=1))
    return (value_sum[None], proj_sum[None], table_sum[None])


def solution(mesh):
    return jax.shard_map(
        per_device,
        mesh=mesh,
        in_specs=(
            P(None, "dp", None),
            P(None, "dp", None),
            P(),
            P(),
            P(),
            P("section", None, None),
            P("section", None, None),
            P("section", None, None),
        ),
        out_specs=(P("section", "dp", None), P("section", "dp", None), P("section", None, "dp")),
        check_vma=False,
    )
```
